32 devices in a mesh: pts: 8 (over z, y), hrs: 4 (over x, core).
Axes of the slice: x: 2, y: 2, z: 4, core: 2. Of those that a mesh axis runs over, the one named last changes fastest.
Arguments:
- fields: float32 [512, 65536], P(('pts', 'hrs')), may hold values from -2000 to 2000, as said below
- probes: float32 [256, 512], replicated, may hold values from -0.25 to 0.25
Outputs:
- basis_rows: float32 [256, 65536], P(None, ('pts', 'hrs'))
- coeffs: float32 [256, 512], replicated
The draws below stay inside these ranges and needn't reach their ends.
Inputs may be any that keep to these rules, and one draw needn't show every extreme that they name: `fields`: every hour and every grid point carries its own scale, and the values are real-valued and never all zero.
All inputs are finite; a program needn't handle non-finite values.
Results may differ from the reference program's by a relative error of at most 0.00017.
Values sent between devices are 32-bit elements; how exact they have to be, the bound alone decides.
A program may use at most 64 MiB of HBM per device.

```python
import jax
import jax.numpy as jnp
from jax import lax

K = 256
HOURS = 512
POINTS = 65536


def draw_fields(key, part):
    keys_all = jax.random.split(jax.random.fold_in(key, 11), 3)
    point_scale = 10.0 ** jax.random.uniform(keys_all[1], (1, POINTS), dtype=jnp.float32)
    lat_ramp = 1.0 + 2.0 * jnp.arange(POINTS, dtype=jnp.float32)[None, :] / (POINTS - 1)
    hour_scale = 10.0 ** jax.random.uniform(keys_all[0], (HOURS, 1), dtype=jnp.float32)
    noise_part = jnp.clip(jax.random.normal(keys_all[2], (HOURS, POINTS), dtype=jnp.float32), -4.0, 4.0)
    return hour_scale * point_scale * lat_ramp * noise_part


def gaussian(own_key, extent, width, most, held_as=jnp.bfloat16):
    values = width * jax.random.normal(own_key, extent, jnp.float32)
    return jnp.clip(values, min=-most, max=most).astype(held_as)


def setup_inputs(seed: int = 0) -> dict:
    key_of = jax.random.split(jax.random.key(seed), 3)
    fields = draw_fields(jax.random.fold_in(key_of[2], 71), 0)
    probes = gaussian(key_of[1], (K, HOURS), HOURS ** -0.5, 0.25, jnp.float32)
    return {"fields": fields, "probes": probes}


highest = lax.Precision.HIGHEST

def reference(fields, probes):
    n_points = fields.shape[1]
    sketched = jnp.dot(probes.astype(jnp.float32), fields.astype(jnp.float32), precision=highest, preferred_element_type=jnp.float32)
    gram = lax.dot_general(sketched.astype(jnp.float32), sketched.astype(jnp.float32), (((1,), (1,)), ((), ())), precision=highest, preferred_element_type=jnp.float32) / n_points
    lower = jnp.linalg.cholesky(gram)
    basis_rows = lax.linalg.triangular_solve(lower, sketched, left_side=True, lower=True)
    coeffs = lax.dot_general(basis_rows.astype(jnp.float32), fields.astype(jnp.float32), (((1,), (1,)), ((), ())), precision=highest, preferred_element_type=jnp.float32) / n_points
    return (basis_rows, coeffs)
```

```python
import functools

import jax
import jax.numpy as jnp
from jax import lax
from jax.experimental import pallas as pl
from jax.experimental.pallas import tpu as pltpu
from jax.sharding import PartitionSpec as P

HI = lax.Precision.HIGHEST

def mm(a, b, dims):
    return lax.dot_general(a, b, (dims, ((), ())), precision=HI, preferred_element_type=jnp.float32)

def invert_block(block):
    b = block.shape[0]
    rows = lax.broadcasted_iota(jnp.int32, (b, 2 * b), 0)
    cols = lax.broadcasted_iota(jnp.int32, (b, 2 * b), 1)
    eye = (rows + b == cols).astype(jnp.float32)
    m = jnp.concatenate([block, eye[:, b:]], axis=1)
    strips = [m[8 * s:8 * s + 8] for s in range(b // 8)]
    srow = lax.broadcasted_iota(jnp.int32, (8, 2 * b), 0)
    for j in range(b - 1):
        s0, r = divmod(j, 8)
        pivot = strips[s0][r:r + 1, :]
        inv = 1.0 / pivot[:, j:j + 1]
        scaled = pivot * inv
        for s in range(s0, b // 8):
            f = strips[s][:, j:j + 1]
            if s == s0:
                if r == 7:
                    continue
                f = jnp.where(srow[:, :1] > r, f, 0.0)
            strips[s] = strips[s] - f * scaled
    m = jnp.concatenate(strips, axis=0)
    d = jnp.sum(jnp.where(rows == cols, m, 0.0), axis=1, keepdims=True)
    return m[:, b:] * lax.rsqrt(d)

def factor_kernel(cross_ref, probes_ref, sk_ref, basis_ref, coeffs_ref, aug, winv):
    k = cross_ref.shape[0]
    b = 64
    aug[:, :k] = mm(cross_ref[...], probes_ref[...], ((1,), (1,)))
    rows = lax.broadcasted_iota(jnp.int32, (k, k), 0)
    cols = lax.broadcasted_iota(jnp.int32, (k, k), 1)
    aug[:, k:] = (rows == cols).astype(jnp.float32)
    for i in range(k // b):
        lo, hi = i * b, (i + 1) * b
        w = invert_block(aug[lo:hi, lo:hi])
        done = mm(w, aug[lo:hi, :], ((1,), (0,)))
        winv[lo:hi, :] = done[:, k:]
        if hi < k:
            aug[hi:, :] = aug[hi:, :] - mm(done[:, hi:k], done, ((0,), (0,)))
    w = winv[...]
    coeffs_ref[...] = mm(w, cross_ref[...], ((1,), (0,)))
    n = sk_ref.shape[1]
    @pl.loop(0, n // 512)
    def _(t):
        c = pl.ds(pl.multiple_of(t * 512, 512), 512)
        basis_ref[:, c] = mm(w, sk_ref[:, c], ((1,), (0,)))

def finish(cross, probes, sk):
    k = cross.shape[0]
    v = pl.BlockSpec(memory_space=pltpu.VMEM)
    return pl.pallas_call(factor_kernel,
        out_shape=(jax.ShapeDtypeStruct(sk.shape, jnp.float32), jax.ShapeDtypeStruct(cross.shape, jnp.float32)),
        in_specs=[v, v, v], out_specs=(v, v),
        scratch_shapes=[pltpu.VMEM((k, 2 * k), jnp.float32), pltpu.VMEM((k, k), jnp.float32)],
        name="factor")(cross, probes, sk)


def sum_kernel(n_pts, n_hrs, x_ref, out_ref, got1, part, got2, s1, r1, s2, r2, s3, r3, s4, r4):
    pts, hrs = lax.axis_index("pts"), lax.axis_index("hrs")
    rows, width = x_ref.shape
    q = rows // n_hrs
    cols = q * width // (8 * n_pts)
    per_row = width // cols

    def peer_hrs(o):
        return lax.rem(hrs + o, n_hrs)

    def peer_pts(o):
        return lax.rem(pts + o, n_pts)

    def tile(p):
        return (
            pl.ds(pl.multiple_of((p // per_row) * 8, 8), 8),
            pl.ds(pl.multiple_of(lax.rem(p, per_row) * cols, 128), cols),
        )

    barrier = pltpu.get_barrier_semaphore()
    for o in range(1, n_hrs):
        pl.semaphore_signal(barrier, inc=1, device_id=(pts, peer_hrs(o)), device_id_type=pl.DeviceIdType.MESH)
    for o in range(1, n_pts):
        pl.semaphore_signal(barrier, inc=1, device_id=(peer_pts(o), hrs), device_id_type=pl.DeviceIdType.MESH)
    pl.semaphore_wait(barrier, n_hrs + n_pts - 2)

    def send(src, dst, ss, rs, device):
        copy = pltpu.make_async_remote_copy(
            src_ref=src, dst_ref=dst, send_sem=ss, recv_sem=rs,
            device_id=device, device_id_type=pl.DeviceIdType.MESH,
        )
        copy.start()
        return copy

    mine = pl.ds(pl.multiple_of(hrs * q, 8), q)
    copies = []
    for o in range(1, n_hrs):
        t = peer_hrs(o)
        src = x_ref.at[pl.ds(pl.multiple_of(t * q, 8), q)]
        copies.append(send(src, got1.at[o - 1], s1.at[o - 1], r1.at[o - 1], (pts, t)))
    total = x_ref[mine, :]
    for o, copy in enumerate(copies):
        copy.wait_recv()
        total = total + got1[o]
    part[...] = total

    copies2 = []
    for o in range(1, n_pts):
        t = peer_pts(o)
        copies2.append(send(part.at[tile(t)], got2.at[o - 1], s2.at[o - 1], r2.at[o - 1], (t, hrs)))
    total = part[tile(pts)]
    for o, copy in enumerate(copies2):
        copy.wait_recv()
        total = total + got2[o]
    tr, tc = tile(pts)
    own = (pl.ds(pl.multiple_of(hrs * q + (pts // per_row) * 8, 8), 8), tc)
    out_ref[own] = total

    copies3 = []
    for o in range(1, n_pts):
        t = peer_pts(o)
        copies3.append(send(out_ref.at[own], out_ref.at[own], s3.at[o - 1], r3.at[o - 1], (t, hrs)))
    for copy in copies3:
        copy.wait_recv()
    copies4 = []
    for o in range(1, n_hrs):
        t = peer_hrs(o)
        copies4.append(send(out_ref.at[mine], out_ref.at[mine], s4.at[o - 1], r4.at[o - 1], (pts, t)))
    for copy in copies4:
        copy.wait_recv()
    for copy in copies + copies2 + copies3 + copies4:
        copy.wait_send()


def sum_all(x, n_pts, n_hrs):
    rows, width = x.shape
    q = rows // n_hrs
    cols = q * width // (8 * n_pts)
    v = pl.BlockSpec(memory_space=pltpu.VMEM)
    dma = pltpu.SemaphoreType.DMA
    return pl.pallas_call(
        functools.partial(sum_kernel, n_pts, n_hrs),
        out_shape=jax.ShapeDtypeStruct(x.shape, jnp.float32),
        in_specs=[v],
        out_specs=v,
        scratch_shapes=[
            pltpu.VMEM((n_hrs - 1, q, width), jnp.float32),
            pltpu.VMEM((q, width), jnp.float32),
            pltpu.VMEM((n_pts - 1, 8, cols), jnp.float32),
            dma((n_hrs - 1,)), dma((n_hrs - 1,)),
            dma((n_pts - 1,)), dma((n_pts - 1,)),
            dma((n_pts - 1,)), dma((n_pts - 1,)),
            dma((n_hrs - 1,)), dma((n_hrs - 1,)),
        ],
        compiler_params=pltpu.CompilerParams(collective_id=0, has_side_effects=True),
        name="sum_all",
    )(x)


def on_device(fields, probes):
    n_pts = lax.axis_size("pts")
    n_hrs = lax.axis_size("hrs")
    panels = lax.all_to_all(fields, ("pts", "hrs"), split_axis=1, concat_axis=0, tiled=True)
    n_points = panels.shape[1] * n_pts * n_hrs
    sketched = jnp.dot(probes, panels, precision=HI, preferred_element_type=jnp.float32)
    cross = sum_all(mm(sketched, panels, ((1,), (1,))) / n_points, n_pts, n_hrs)
    return finish(cross, probes, sketched)


def solution(mesh):
    return jax.shard_map(
        on_device,
        mesh=mesh,
        in_specs=(P(("pts", "hrs"), None), P()),
        out_specs=(P(None, ("pts", "hrs")), P()),
        check_vma=False,
    )
```

```python
import functools

import jax
import jax.numpy as jnp
from jax import lax
from jax.experimental import pallas as pl
from jax.experimental.pallas import tpu as pltpu
from jax.sharding import PartitionSpec as P

HI = lax.Precision.HIGHEST

def mm(a, b, dims):
    return lax.dot_general(a, b, (dims, ((), ())), precision=HI, preferred_element_type=jnp.float32)

def invert_block(block):
    b = block.shape[0]
    rows = lax.broadcasted_iota(jnp.int32, (b, 2 * b), 0)
    cols = lax.broadcasted_iota(jnp.int32, (b, 2 * b), 1)
    eye = (rows + b == cols).astype(jnp.float32)
    m = jnp.concatenate([block, eye[:, b:]], axis=1)
    strips = [m[8 * s:8 * s + 8] for s in range(b // 8)]
    srow = lax.broadcasted_iota(jnp.int32, (8, 2 * b), 0)
    for j in range(b - 1):
        s0, r = divmod(j, 8)
        pivot = strips[s0][r:r + 1, :]
        inv = 1.0 / pivot[:, j:j + 1]
        scaled = pivot * inv
        for s in range(s0, b // 8):
            f = strips[s][:, j:j + 1]
            if s == s0:
                if r == 7:
                    continue
                f = jnp.where(srow[:, :1] > r, f, 0.0)
            strips[s] = strips[s] - f * scaled
    m = jnp.concatenate(strips, axis=0)
    d = jnp.sum(jnp.where(rows == cols, m, 0.0), axis=1, keepdims=True)
    return m[:, b:] * lax.rsqrt(d)

def factor_kernel(cross_ref, probes_ref, sk_ref, basis_ref, coeffs_ref, aug, winv):
    k = cross_ref.shape[0]
    b = 64
    aug[:, :k] = mm(cross_ref[...], probes_ref[...], ((1,), (1,)))
    rows = lax.broadcasted_iota(jnp.int32, (k, k), 0)
    cols = lax.broadcasted_iota(jnp.int32, (k, k), 1)
    aug[:, k:] = (rows == cols).astype(jnp.float32)
    for i in range(k // b):
        lo, hi = i * b, (i + 1) * b
        w = invert_block(aug[lo:hi, lo:hi])
        done = mm(w, aug[lo:hi, :], ((1,), (0,)))
        winv[lo:hi, :] = done[:, k:]
        if hi < k:
            aug[hi:, :] = aug[hi:, :] - mm(done[:, hi:k], done, ((0,), (0,)))
    w = winv[...]
    coeffs_ref[...] = mm(w, cross_ref[...], ((1,), (0,)))
    n = sk_ref.shape[1]
    @pl.loop(0, n // 512)
    def _(t):
        c = pl.ds(pl.multiple_of(t * 512, 512), 512)
        basis_ref[:, c] = mm(w, sk_ref[:, c], ((1,), (0,)))

def finish(cross, probes, sk):
    k = cross.shape[0]
    v = pl.BlockSpec(memory_space=pltpu.VMEM)
    return pl.pallas_call(factor_kernel,
        out_shape=(jax.ShapeDtypeStruct(sk.shape, jnp.float32), jax.ShapeDtypeStruct(cross.shape, jnp.float32)),
        in_specs=[v, v, v], out_specs=(v, v),
        scratch_shapes=[pltpu.VMEM((k, 2 * k), jnp.float32), pltpu.VMEM((k, k), jnp.float32)],
        name="factor")(cross, probes, sk)


def sum_kernel(n_pts, n_hrs, x_ref, out_ref, got1, part, got2, s1, r1, s2, r2, s3, r3, s4, r4):
    pts, hrs = lax.axis_index("pts"), lax.axis_index("hrs")
    rows, width = x_ref.shape
    q = rows // n_hrs
    cols = q * width // (8 * n_pts)
    per_row = width // cols

    def peer_hrs(o):
        return lax.rem(hrs + o, n_hrs)

    def peer_pts(o):
        return lax.rem(pts + o, n_pts)

    def tile(p):
        return (
            pl.ds(pl.multiple_of((p // per_row) * 8, 8), 8),
            pl.ds(pl.multiple_of(lax.rem(p, per_row) * cols, 128), cols),
        )

    barrier = pltpu.get_barrier_semaphore()
    for o in range(1, n_hrs):
        pl.semaphore_signal(barrier, inc=1, device_id=(pts, peer_hrs(o)), device_id_type=pl.DeviceIdType.MESH)
    for o in range(1, n_pts):
        pl.semaphore_signal(barrier, inc=1, device_id=(peer_pts(o), hrs), device_id_type=pl.DeviceIdType.MESH)
    pl.semaphore_wait(barrier, n_hrs + n_pts - 2)

    def send(src, dst, ss, rs, device):
        copy = pltpu.make_async_remote_copy(
            src_ref=src, dst_ref=dst, send_sem=ss, recv_sem=rs,
            device_id=device, device_id_type=pl.DeviceIdType.MESH,
        )
        copy.start()
        return copy

    mine = pl.ds(pl.multiple_of(hrs * q, 8), q)
    copies = []
    for o in range(1, n_hrs):
        t = peer_hrs(o)
        src = x_ref.at[pl.ds(pl.multiple_of(t * q, 8), q)]
        copies.append(send(src, got1.at[o - 1], s1.at[o - 1], r1.at[o - 1], (pts, t)))
    total = x_ref[mine, :]
    for o, copy in enumerate(copies):
        copy.wait_recv()
        total = total + got1[o]
    part[...] = total

    copies2 = []
    for o in range(1, n_pts):
        t = peer_pts(o)
        copies2.append(send(part.at[tile(t)], got2.at[o - 1], s2.at[o - 1], r2.at[o - 1], (t, hrs)))
    total = part[tile(pts)]
    for o, copy in enumerate(copies2):
        copy.wait_recv()
        total = total + got2[o]
    tr, tc = tile(pts)
    own = (pl.ds(pl.multiple_of(hrs * q + (pts // per_row) * 8, 8), 8), tc)
    out_ref[own] = total

    copies3 = []
    for o in range(1, n_pts):
        t = peer_pts(o)
        copies3.append(send(out_ref.at[own], out_ref.at[own], s3.at[o - 1], r3.at[o - 1], (t, hrs)))
    for copy in copies3:
        copy.wait_recv()
    copies4 = []
    for o in range(1, n_hrs):
        t = peer_hrs(o)
        copies4.append(send(out_ref.at[mine], out_ref.at[mine], s4.at[o - 1], r4.at[o - 1], (pts, t)))
    for copy in copies4:
        copy.wait_recv()
    for copy in copies + copies2 + copies3 + copies4:
        copy.wait_send()


def sum_all(x, n_pts, n_hrs):
    rows, width = x.shape
    q = rows // n_hrs
    cols = q * width // (8 * n_pts)
    v = pl.BlockSpec(memory_space=pltpu.VMEM)
    dma = pltpu.SemaphoreType.DMA
    return pl.pallas_call(
        functools.partial(sum_kernel, n_pts, n_hrs),
        out_shape=jax.ShapeDtypeStruct(x.shape, jnp.float32),
        in_specs=[v],
        out_specs=v,
        scratch_shapes=[
            pltpu.VMEM((n_hrs - 1, q, width), jnp.float32),
            pltpu.VMEM((q, width), jnp.float32),
            pltpu.VMEM((n_pts - 1, 8, cols), jnp.float32),
            dma((n_hrs - 1,)), dma((n_hrs - 1,)),
            dma((n_pts - 1,)), dma((n_pts - 1,)),
            dma((n_pts - 1,)), dma((n_pts - 1,)),
            dma((n_hrs - 1,)), dma((n_hrs - 1,)),
        ],
        compiler_params=pltpu.CompilerParams(collective_id=0, has_side_effects=True),
        name="sum_all",
    )(x)


def gather_kernel(n_pts, n_hrs, chunks, n_points, fields_ref, probes_ref, sk_ref, cross_ref, panels, flat, own_sem, send_sem, recv_sem):
    pts, hrs = lax.axis_index("pts"), lax.axis_index("hrs")
    n = n_pts * n_hrs
    me = pts * n_hrs + hrs
    rows = fields_ref.shape[0]
    width = panels.shape[3]
    local = width * chunks

    def split(o):
        t = lax.rem(me + o, n)
        return t, t // n_hrs, lax.rem(t, n_hrs)

    barrier = pltpu.get_barrier_semaphore()

    @pl.loop(1, n)
    def _(o):
        _, tp, th = split(o)
        pl.semaphore_signal(barrier, inc=1, device_id=(tp, th), device_id_type=pl.DeviceIdType.MESH)

    pl.semaphore_wait(barrier, n - 1)

    def source(t, c):
        return fields_ref.at[:, pl.ds(pl.multiple_of(t * local + c * width, 128), width)]

    owns = []
    for c in range(chunks):
        @pl.loop(1, n)
        def _(o):
            t, tp, th = split(o)
            pltpu.make_async_remote_copy(
                src_ref=source(t, c), dst_ref=panels.at[c, me], send_sem=send_sem.at[c], recv_sem=recv_sem.at[c],
                device_id=(tp, th), device_id_type=pl.DeviceIdType.MESH,
            ).start()

        own = pltpu.make_async_copy(source(me, c), panels.at[c, me], own_sem.at[c])
        own.start()
        owns.append(own)

    for c in range(chunks):
        owns[c].wait()
        most = panels.at[c, pl.ds(0, n - 1)]
        pltpu.make_async_copy(most, most, recv_sem.at[c]).wait()
        if rows % 8 == 0:
            block = panels[c].reshape(n * rows, width)
        else:
            for d in range(n):
                flat[d * rows:(d + 1) * rows, :] = panels[c, d]
            block = flat[...]
        sk = mm(probes_ref[...], block, ((1,), (0,)))
        sk_ref[:, c * width:(c + 1) * width] = sk
        term = mm(sk, block, ((1,), (1,)))
        cross_ref[...] = term if c == 0 else cross_ref[...] + term
    cross_ref[...] = cross_ref[...] / n_points
    for c in range(chunks):
        most = panels.at[c, pl.ds(0, n - 1)]
        pltpu.make_async_copy(most, most, send_sem.at[c]).wait()


def gather(fields, probes, n_pts, n_hrs, chunks):
    k, hours = probes.shape
    rows, n_points = fields.shape
    n = n_pts * n_hrs
    local = n_points // n
    width = local // chunks
    v = pl.BlockSpec(memory_space=pltpu.VMEM)
    dma = pltpu.SemaphoreType.DMA
    return pl.pallas_call(
        functools.partial(gather_kernel, n_pts, n_hrs, chunks, n_points),
        out_shape=(jax.ShapeDtypeStruct((k, local), jnp.float32), jax.ShapeDtypeStruct((k, hours), jnp.float32)),
        in_specs=[pl.BlockSpec(memory_space=pl.ANY), v],
        out_specs=(v, v),
        scratch_shapes=[
            pltpu.VMEM((chunks, n, rows, width), jnp.float32),
            pltpu.VMEM((hours, width) if rows % 8 else (8, 128), jnp.float32),
            dma((chunks,)), dma((chunks,)), dma((chunks,)),
        ],
        compiler_params=pltpu.CompilerParams(collective_id=1, has_side_effects=True),
        name="gather",
    )(fields, probes)


def on_device(fields, probes):
    n_pts = lax.axis_size("pts")
    n_hrs = lax.axis_size("hrs")
    sketched, cross = gather(fields, probes, n_pts, n_hrs, 4)
    return finish(sum_all(cross, n_pts, n_hrs), probes, sketched)


def solution(mesh):
    return jax.shard_map(
        on_device,
        mesh=mesh,
        in_specs=(P(("pts", "hrs"), None), P()),
        out_specs=(P(None, ("pts", "hrs")), P()),
        check_vma=False,
    )
```

```python
import functools

import jax
import jax.numpy as jnp
from jax import lax
from jax.experimental import pallas as pl
from jax.experimental.pallas import tpu as pltpu
from jax.sharding import PartitionSpec as P

HI = lax.Precision.HIGHEST

def mm(a, b, dims):
    return lax.dot_general(a, b, (dims, ((), ())), precision=HI, preferred_element_type=jnp.float32)

def invert_block(block, group):
    b = block.shape[0]
    shape = (8, 2 * b)
    rows = lax.broadcasted_iota(jnp.int32, (b, 2 * b), 0)
    cols = lax.broadcasted_iota(jnp.int32, (b, 2 * b), 1)
    eye = (rows + b == cols).astype(jnp.float32)
    m = jnp.concatenate([block, eye[:, b:]], axis=1)
    strips = [m[8 * s:8 * s + 8] for s in range(b // 8)]
    srow = lax.broadcasted_iota(jnp.int32, shape, 0)
    for j in range(0, b, group):
        s0, r0 = divmod(j, 8)
        strip = strips[s0]
        pivots = [jnp.broadcast_to(strip[r0 + r:r0 + r + 1, :], shape) for r in range(group)]
        corner = [
            [jnp.broadcast_to(strip[r0 + r:r0 + r + 1, j + c:j + c + 1], shape) for c in range(r + 1)]
            for r in range(group)
        ]
        ratio = [[None] * group for _ in range(group)]
        scaled = []
        for r in range(group):
            inv = 1.0 / corner[r][r]
            for lo in range(r + 1, group):
                ratio[lo][r] = corner[lo][r] * inv
            for lo in range(r + 1, group):
                for c in range(r + 1, lo + 1):
                    corner[lo][c] = corner[lo][c] - ratio[lo][r] * corner[c][r]
                pivots[lo] = pivots[lo] - ratio[lo][r] * pivots[r]
            scaled.append(pivots[r] * inv)
        for s in range(s0, b // 8):
            if s == s0 and r0 + group == 8:
                new = strips[s]
            else:
                held = strips[s]
                f = []
                new = held
                for r in range(group):
                    fr = jnp.broadcast_to(held[:, j + r:j + r + 1], shape)
                    for c in range(r):
                        fr = fr - ratio[r][c] * f[c]
                    f.append(fr)
                    new = new - fr * scaled[r]
                if s == s0:
                    new = jnp.where(srow >= r0 + group, new, held)
            if s == s0:
                for r in range(group):
                    new = jnp.where(srow == r0 + r, pivots[r], new)
            strips[s] = new
    m = jnp.concatenate(strips, axis=0)
    d = jnp.sum(jnp.where(rows == cols, m, 0.0), axis=1, keepdims=True)
    return m[:, b:] * lax.rsqrt(d)


def factor_kernel(cross_ref, probes_ref, sk_ref, basis_ref, coeffs_ref, aug, winv):
    k = cross_ref.shape[0]
    b = 64
    aug[:, :k] = mm(cross_ref[...], probes_ref[...], ((1,), (1,)))
    rows = lax.broadcasted_iota(jnp.int32, (k, k), 0)
    cols = lax.broadcasted_iota(jnp.int32, (k, k), 1)
    aug[:, k:] = (rows == cols).astype(jnp.float32)
    for i in range(k // b):
        lo, hi = i * b, (i + 1) * b
        w = invert_block(aug[lo:hi, lo:hi], 8)
        done = mm(w, aug[lo:hi, :], ((1,), (0,)))
        winv[lo:hi, :] = done[:, k:]
        if hi < k:
            aug[hi:, :] = aug[hi:, :] - mm(done[:, hi:k], done, ((0,), (0,)))
    w = winv[...]
    coeffs_ref[...] = mm(w, cross_ref[...], ((1,), (0,)))
    n = sk_ref.shape[1]
    @pl.loop(0, n // 512)
    def _(t):
        c = pl.ds(pl.multiple_of(t * 512, 512), 512)
        basis_ref[:, c] = mm(w, sk_ref[:, c], ((1,), (0,)))

def finish(cross, probes, sk):
    k = cross.shape[0]
    v = pl.BlockSpec(memory_space=pltpu.VMEM)
    return pl.pallas_call(factor_kernel,
        out_shape=(jax.ShapeDtypeStruct(sk.shape, jnp.float32), jax.ShapeDtypeStruct(cross.shape, jnp.float32)),
        in_specs=[v, v, v], out_specs=(v, v),
        scratch_shapes=[pltpu.VMEM((k, 2 * k), jnp.float32), pltpu.VMEM((k, k), jnp.float32)],
        name="factor")(cross, probes, sk)


def sum_kernel(n_pts, n_hrs, lanes, cols, x_ref, out_ref, got1, part, got2, s1, r1, s2, r2, s3, r3, s4, r4):
    pts, hrs = lax.axis_index("pts"), lax.axis_index("hrs")
    rows, width = x_ref.shape
    q = rows // n_hrs
    parts = width // lanes
    per_row = lanes // cols

    def peer_hrs(o):
        return lax.rem(hrs + o, n_hrs)

    def peer_pts(o):
        return lax.rem(pts + o, n_pts)

    def tile(h, p, first=0):
        return (
            pl.ds(pl.multiple_of(first + (p // per_row) * 8, 8), 8),
            pl.ds(pl.multiple_of(h * lanes + lax.rem(p, per_row) * cols, 128), cols),
        )

    barrier = pltpu.get_barrier_semaphore()
    for o in range(1, n_hrs):
        pl.semaphore_signal(barrier, inc=1, device_id=(pts, peer_hrs(o)), device_id_type=pl.DeviceIdType.MESH)
    for o in range(1, n_pts):
        pl.semaphore_signal(barrier, inc=1, device_id=(peer_pts(o), hrs), device_id_type=pl.DeviceIdType.MESH)
    pl.semaphore_wait(barrier, n_hrs + n_pts - 2)

    started = []

    def send(src, dst, ss, rs, device):
        copy = pltpu.make_async_remote_copy(
            src_ref=src, dst_ref=dst, send_sem=ss, recv_sem=rs,
            device_id=device, device_id_type=pl.DeviceIdType.MESH,
        )
        copy.start()
        started.append(copy)
        return copy

    def along(h):
        return pl.ds(h * lanes, lanes)

    mine = pl.ds(pl.multiple_of(hrs * q, 8), q)
    first, second, third, fourth = [], [], [], []
    for h in range(parts):
        copies = []
        for o in range(1, n_hrs):
            t = peer_hrs(o)
            src = x_ref.at[pl.ds(pl.multiple_of(t * q, 8), q), along(h)]
            copies.append(send(src, got1.at[h, o - 1], s1.at[h, o - 1], r1.at[h, o - 1], (pts, t)))
        first.append(copies)
    for h in range(parts):
        total = x_ref[mine, along(h)]
        for o, copy in enumerate(first[h]):
            copy.wait_recv()
            total = total + got1[h, o]
        part[:, along(h)] = total
        copies = []
        for o in range(1, n_pts):
            t = peer_pts(o)
            copies.append(send(part.at[tile(h, t)], got2.at[h, o - 1], s2.at[h, o - 1], r2.at[h, o - 1], (t, hrs)))
        second.append(copies)
    for h in range(parts):
        total = part[tile(h, pts)]
        for o, copy in enumerate(second[h]):
            copy.wait_recv()
            total = total + got2[h, o]
        own = tile(h, pts, hrs * q)
        out_ref[own] = total
        copies = []
        for o in range(1, n_pts):
            t = peer_pts(o)
            copies.append(send(out_ref.at[own], out_ref.at[own], s3.at[h, o - 1], r3.at[h, o - 1], (t, hrs)))
        third.append(copies)
    for h in range(parts):
        for copy in third[h]:
            copy.wait_recv()
        copies = []
        block = out_ref.at[mine, along(h)]
        for o in range(1, n_hrs):
            copies.append(send(block, block, s4.at[h, o - 1], r4.at[h, o - 1], (pts, peer_hrs(o))))
        fourth.append(copies)
    for copies in fourth:
        for copy in copies:
            copy.wait_recv()
    for copy in started:
        copy.wait_send()


def sum_all(x, n_pts, n_hrs, parts=2):
    rows, width = x.shape
    q = rows // n_hrs
    parts = max(1, min(parts, q * width // (8 * 128 * n_pts)))
    lanes = width // parts
    cols = q * lanes // (8 * n_pts)
    v = pl.BlockSpec(memory_space=pltpu.VMEM)
    dma = pltpu.SemaphoreType.DMA
    return pl.pallas_call(
        functools.partial(sum_kernel, n_pts, n_hrs, lanes, cols),
        out_shape=jax.ShapeDtypeStruct(x.shape, jnp.float32),
        in_specs=[v],
        out_specs=v,
        scratch_shapes=[
            pltpu.VMEM((parts, n_hrs - 1, q, lanes), jnp.float32),
            pltpu.VMEM((q, width), jnp.float32),
            pltpu.VMEM((parts, n_pts - 1, 8, cols), jnp.float32),
            dma((parts, n_hrs - 1)), dma((parts, n_hrs - 1)),
            dma((parts, n_pts - 1)), dma((parts, n_pts - 1)),
            dma((parts, n_pts - 1)), dma((parts, n_pts - 1)),
            dma((parts, n_hrs - 1)), dma((parts, n_hrs - 1)),
        ],
        compiler_params=pltpu.CompilerParams(collective_id=0, has_side_effects=True),
        name="sum_all",
    )(x)


def gather_kernel(n_pts, n_hrs, chunks, n_points, fields_ref, probes_ref, sk_ref, cross_ref, panels, flat, own_sem, send_sem, recv_sem):
    pts, hrs = lax.axis_index("pts"), lax.axis_index("hrs")
    n = n_pts * n_hrs
    me = pts * n_hrs + hrs
    rows = fields_ref.shape[0]
    width = panels.shape[3]
    local = width * chunks

    def split(o):
        t = lax.rem(me + o, n)
        return t, t // n_hrs, lax.rem(t, n_hrs)

    barrier = pltpu.get_barrier_semaphore()

    @pl.loop(1, n)
    def _(o):
        _, tp, th = split(o)
        pl.semaphore_signal(barrier, inc=1, device_id=(tp, th), device_id_type=pl.DeviceIdType.MESH)

    pl.semaphore_wait(barrier, n - 1)

    def source(t, c):
        return fields_ref.at[:, pl.ds(pl.multiple_of(t * local + c * width, 128), width)]

    owns = []
    for c in range(chunks):
        @pl.loop(1, n)
        def _(o):
            t, tp, th = split(o)
            pltpu.make_async_remote_copy(
                src_ref=source(t, c), dst_ref=panels.at[c, me], send_sem=send_sem.at[c], recv_sem=recv_sem.at[c],
                device_id=(tp, th), device_id_type=pl.DeviceIdType.MESH,
            ).start()

        own = pltpu.make_async_copy(source(me, c), panels.at[c, me], own_sem.at[c])
        own.start()
        owns.append(own)

    for c in range(chunks):
        owns[c].wait()
        most = panels.at[c, pl.ds(0, n - 1)]
        pltpu.make_async_copy(most, most, recv_sem.at[c]).wait()
        if rows % 8 == 0:
            block = panels[c].reshape(n * rows, width)
        else:
            for d in range(n):
                flat[d * rows:(d + 1) * rows, :] = panels[c, d]
            block = flat[...]
        sk = mm(probes_ref[...], block, ((1,), (0,)))
        sk_ref[:, c * width:(c + 1) * width] = sk
        term = mm(sk, block, ((1,), (1,)))
        cross_ref[...] = term if c == 0 else cross_ref[...] + term
    cross_ref[...] = cross_ref[...] / n_points
    for c in range(chunks):
        most = panels.at[c, pl.ds(0, n - 1)]
        pltpu.make_async_copy(most, most, send_sem.at[c]).wait()


def gather(fields, probes, n_pts, n_hrs, chunks):
    k, hours = probes.shape
    rows, n_points = fields.shape
    n = n_pts * n_hrs
    local = n_points // n
    width = local // chunks
    v = pl.BlockSpec(memory_space=pltpu.VMEM)
    dma = pltpu.SemaphoreType.DMA
    return pl.pallas_call(
        functools.partial(gather_kernel, n_pts, n_hrs, chunks, n_points),
        out_shape=(jax.ShapeDtypeStruct((k, local), jnp.float32), jax.ShapeDtypeStruct((k, hours), jnp.float32)),
        in_specs=[pl.BlockSpec(memory_space=pl.ANY), v],
        out_specs=(v, v),
        scratch_shapes=[
            pltpu.VMEM((chunks, n, rows, width), jnp.float32),
            pltpu.VMEM((hours, width) if rows % 8 else (8, 128), jnp.float32),
            dma((chunks,)), dma((chunks,)), dma((chunks,)),
        ],
        compiler_params=pltpu.CompilerParams(collective_id=1, has_side_effects=True),
        name="gather",
    )(fields, probes)


def on_device(fields, probes):
    n_pts = lax.axis_size("pts")
    n_hrs = lax.axis_size("hrs")
    sketched, cross = gather(fields, probes, n_pts, n_hrs, 4)
    return finish(sum_all(cross, n_pts, n_hrs), probes, sketched)


def solution(mesh):
    return jax.shard_map(
        on_device,
        mesh=mesh,
        in_specs=(P(("pts", "hrs"), None), P()),
        out_specs=(P(None, ("pts", "hrs")), P()),
        check_vma=False,
    )
```
